8 devices in a mesh: seqs: 1 (over z), rows: 2 (over y), states: 4 (over x, core).
Axes of the slice: x: 2, y: 2, z: 1, core: 2. Of those that a mesh axis runs over, the one named last changes fastest.
Arguments:
- trans_mat: bfloat16 [16384, 2, 8192], P('rows', None, 'states')
- emit_mat: bfloat16 [16384, 10000], P(('rows', 'states'))
- init_dist: float32 [16384], P(('rows', 'states'))
- tokens: int32 [64, 32], P('seqs')
- lengths: int32 [64], P('seqs')
Outputs:
- output 1: float32 [64], P('seqs')
- output 2: float32 [64, 16384], P('seqs', ('rows', 'states'))
All inputs are finite; a program needn't handle non-finite values.
Results may differ from the reference program's by a relative error of at most 0.001.
Values are sent between devices in bfloat16 or wider.
A program may use at most 1 GiB of HBM per device.

```python
import jax
import jax.numpy as jnp
from jax import lax
import functools

STATES = 16384
VOCAB = 10000
BATCH = 64
STEPS = 32
ROW_SPLIT = 2
DRAW_ROWS = 256


def draw_rows(key, n_cols, sharpness):
    logits = sharpness * jax.random.normal(key, (DRAW_ROWS, n_cols), jnp.float32)
    return jax.nn.softmax(logits, axis=1).astype(jnp.bfloat16)


def draw_sequences(key):
    key_tok, key_len, key_long, key_short = jax.random.split(key, 4)
    tokens = jax.random.randint(key_tok, (BATCH, STEPS), 0, VOCAB, dtype=jnp.int32)
    lengths = jax.random.randint(key_len, (BATCH,), 1, STEPS + 1, dtype=jnp.int32)
    long_row = jax.random.randint(key_long, (), 0, BATCH, dtype=jnp.int32)
    short_row = (long_row + 1 + jax.random.randint(key_short, (), 0, BATCH - 1, dtype=jnp.int32)) % BATCH
    lengths = lengths.at[long_row].set(STEPS).at[short_row].set(1)
    return tokens, lengths


def setup_inputs(seed: int = 0, part: int = 0) -> dict:
    base_key = jax.random.key(seed)
    key_trans, key_emit, key_init, key_seq = jax.random.split(base_key, 4)
    n_blocks = STATES // DRAW_ROWS
    trans_rows = lax.map(functools.partial(draw_rows, n_cols=STATES, sharpness=2.5), jax.random.split(key_trans, n_blocks))
    emit_rows = lax.map(functools.partial(draw_rows, n_cols=VOCAB, sharpness=2.0), jax.random.split(key_emit, n_blocks))
    init_dist = jax.nn.softmax(1.5 * jax.random.normal(key_init, (STATES,), jnp.float32))
    tokens, lengths = draw_sequences(jax.random.fold_in(key_seq, part))
    return {'trans_mat': trans_rows.reshape(STATES, ROW_SPLIT, STATES // ROW_SPLIT), 'emit_mat': emit_rows.reshape(STATES, VOCAB), 'init_dist': init_dist, 'tokens': tokens, 'lengths': lengths}


def emission(emit_mat, step_tok):
    return jnp.take(emit_mat, step_tok, axis=1).T.astype(jnp.float32)


def reference(trans_mat, emit_mat, init_dist, tokens, lengths):
    trans_full = trans_mat.reshape(STATES, STATES)
    first_raw = init_dist[None, :] * emission(emit_mat, tokens[:, 0])
    norm_c = jnp.sum(first_raw, axis=1)
    alpha_init = first_raw / norm_c[:, None]
    loglik_init = jnp.log(norm_c)

    def one_step(state_in, inputs):
        alpha_cur, loglik = state_in
        step_tok, t_index = inputs
        mix_sum = jnp.dot(alpha_cur.astype(jnp.bfloat16), trans_full, preferred_element_type=jnp.float32)
        raw_next = mix_sum * emission(emit_mat, step_tok)
        norm_step = jnp.sum(raw_next, axis=1)
        active = t_index < lengths
        alpha_cur = jnp.where(active[:, None], raw_next / norm_step[:, None], alpha_cur)
        loglik = loglik + jnp.where(active, jnp.log(norm_step), 0.0)
        return (alpha_cur, loglik), None

    scan_out = lax.scan(one_step, (alpha_init, loglik_init), (tokens[:, 1:].T, jnp.arange(1, STEPS)))
    alpha_last, loglik = scan_out[0]
    return loglik, alpha_last
```

```python
import functools

import jax
import jax.numpy as jnp
from jax import lax
from jax.experimental import pallas as pl
from jax.experimental.pallas import tpu as pltpu
from jax.sharding import PartitionSpec as P

MESH = pl.DeviceIdType.MESH
LANES = 128
GROUP = 8


def forward_kernel(
    n_steps, rows, width, piece, chunk, depth,
    a_hbm, emis_hbm, init_ref, len_pack, len_col,
    ll_ref, alpha_ref,
    held, ring, a_bf, gath, y_out, y_in, emis, c_buf, c_acc, inv_b,
    held_sem, ring_sem, emis_sem, y_ss, y_rs, x_ss, x_rs, p_ss, p_rs, f_ss, f_rs, c_ss, c_rs,
    credit_x, credit_p,
):
    n_pieces = width // piece
    n_chunks = width // chunk
    n_held_own = held.shape[0] - n_chunks
    per_chunk = chunk // piece
    k_parts = a_bf.shape[1] // depth
    row = lax.axis_index('rows')
    st = lax.axis_index('states')
    across = lax.rem(st + 2, 4)
    partner = st + 1 - 2 * lax.rem(st, 2)
    other = 1 - row
    me = row * 4 + st
    to_y = {'rows': other}
    to_x = {'states': across}
    to_p = {'states': partner}
    peers = []
    for k in range(1, 8):
        peers.append({'rows': lax.rem(row + k // 4, 2), 'states': lax.rem(st + k % 4, 4)})

    barrier = pltpu.get_barrier_semaphore()
    for peer in peers:
        pl.semaphore_signal(barrier, inc=1, device_id=peer, device_id_type=MESH)

    def held_copy(ch):
        half, c = (other, ch) if ch < n_chunks else (row, ch - n_chunks)
        return pltpu.make_async_copy(a_hbm.at[half, :, pl.ds(c * chunk, chunk)], held.at[ch], held_sem.at[ch])

    def ring_copy(c, k):
        cols = pl.ds(pl.multiple_of(c * chunk, chunk), chunk)
        return pltpu.make_async_copy(a_hbm.at[row, pl.ds(k * depth, depth), cols], ring.at[k], ring_sem.at[k])

    def emis_copy(t, slot):
        return pltpu.make_async_copy(emis_hbm.at[t, pl.ds(0, rows)], emis.at[slot], emis_sem.at[slot])

    def remote(src, dst, ss, rs, dev):
        return pltpu.make_async_remote_copy(src_ref=src, dst_ref=dst, send_sem=ss, recv_sem=rs, device_id=dev, device_id_type=MESH)

    def y_copy(p):
        return remote(y_out.at[p], y_in.at[p], y_ss.at[p], y_rs.at[p], to_y)

    def x_copy(p):
        return remote(gath.at[st, p], gath.at[st, p], x_ss.at[p], x_rs.at[p], to_x)

    def x_arrived(p):
        return remote(gath.at[across, p], gath.at[across, p], x_ss.at[p], x_rs.at[p], to_x)

    def p_copy(p):
        return remote(gath.at[st, p], gath.at[st, p], p_ss.at[p], p_rs.at[p], to_p)

    def p_arrived(p):
        return remote(gath.at[partner, p], gath.at[partner, p], p_ss.at[p], p_rs.at[p], to_p)

    def f_copy(p):
        return remote(gath.at[across, p], gath.at[across, p], f_ss.at[p], f_rs.at[p], to_p)

    def f_arrived(p):
        far = lax.rem(partner + 2, 4)
        return remote(gath.at[far, p], gath.at[far, p], f_ss.at[p], f_rs.at[p], to_p)

    def c_copy(par, k):
        return remote(c_buf.at[par, me], c_buf.at[par, me], c_ss.at[k], c_rs.at[par, k], peers[k - 1])

    def c_arrived(par, k):
        src = lax.rem(row + k // 4, 2) * 4 + lax.rem(st + 4 - k % 4, 4)
        return remote(c_buf.at[par, src], c_buf.at[par, src], c_ss.at[k], c_rs.at[par, k], peers[k - 1])

    emis_copy(0, 0).start()
    for ch in range(held.shape[0]):
        held_copy(ch).start()
    for k in range(k_parts):
        ring_copy(n_held_own, k).start()
    emis_copy(1, 1).start()
    pl.semaphore_wait(barrier, 7)

    lane = lax.broadcasted_iota(jnp.int32, (GROUP, LANES), 1)
    ll_ref[...] = jnp.zeros_like(ll_ref)
    alpha_ref[...] = jnp.zeros_like(alpha_ref)

    def emit_piece(p, value, cols, par):
        r = value * emis[par, :, cols].astype(jnp.float32)
        gath[st, p] = r
        part = r[:, :LANES]
        for j in range(1, piece // LANES):
            part = part + r[:, j * LANES:(j + 1) * LANES]
        c_acc[...] += part
        x_copy(p).start()
        p_copy(p).start()

    def forward(p):
        x_arrived(p).wait_recv()
        f_copy(p).start()

    def finish(t, first_forward):
        par = lax.rem(t, 2)
        pack = jnp.zeros((GROUP, LANES), jnp.float32)
        for i in range(rows // GROUP):
            total = jnp.sum(c_acc[pl.ds(i * GROUP, GROUP), :], axis=1, keepdims=True)
            pack = jnp.where(lane == i, total, pack)
        c_buf[par, me] = pack
        for k in range(1, 8):
            c_copy(par, k).start()
        c_acc[...] = jnp.zeros_like(c_acc)
        for p in range(first_forward, n_pieces):
            forward(p)
        for k in range(1, 8):
            c_arrived(par, k).wait_recv()
        total = c_buf[par, 0]
        for k in range(1, 8):
            total = total + c_buf[par, k]
        ll_ref[...] += jnp.where(t < len_pack[...], jnp.log(total), 0.0)
        inv = 1.0 / total
        for i in range(rows // GROUP):
            inv_b[pl.ds(i * GROUP, GROUP), :] = jnp.broadcast_to(inv[:, i:i + 1], (GROUP, LANES))

        def convert(src, p):
            scale = inv_b[...]
            for j in range(piece // LANES):
                at = pl.multiple_of(src * width + p * piece + j * LANES, LANES)
                a_bf[:, pl.ds(at, LANES)] = (gath[src, p, :, j * LANES:(j + 1) * LANES] * scale).astype(jnp.bfloat16)

        def convert_own(p, _):
            convert(st, p)
            convert(across, p)
            return 0

        lax.fori_loop(0, n_pieces, convert_own, 0)

        def convert_near(p, _):
            p_arrived(p).wait_recv()
            f_arrived(p).wait_recv()
            convert(partner, p)
            convert(lax.rem(partner + 2, 4), p)
            return 0

        lax.fori_loop(0, n_pieces, convert_near, 0)
        for p in range(n_pieces):
            x_copy(p).wait_send()
            p_copy(p).wait_send()
            f_copy(p).wait_send()
        for k in range(1, 8):
            c_copy(par, k).wait_send()

        @pl.when(t < n_steps - 1)
        def _():
            pl.semaphore_signal(credit_x, inc=1, device_id=to_x, device_id_type=MESH)
            pl.semaphore_signal(credit_p, inc=1, device_id=to_p, device_id_type=MESH)

        live = t < len_col[...]
        scale = inv_b[...]
        for p in range(n_pieces):
            for j in range(piece // LANES):
                cols = pl.ds(p * piece + j * LANES, LANES)
                alpha_ref[:, cols] = jnp.where(live, gath[st, p, :, j * LANES:(j + 1) * LANES] * scale, alpha_ref[:, cols])

    c_acc[...] = jnp.zeros_like(c_acc)
    emis_copy(0, 0).wait()
    for p in range(n_pieces):
        cols = pl.ds(p * piece, piece)
        emit_piece(p, jnp.broadcast_to(init_ref[:, cols], (rows, piece)), cols, 0)
    finish(0, 0)

    def one_step(t, _):
        par = lax.rem(t, 2)

        @pl.when(t + 1 < n_steps)
        def _():
            emis_copy(t + 1, 1 - par).start()

        def send_half(c, _):
            @pl.when(t == 1)
            def _():
                for ch in range(n_chunks):
                    @pl.when(c == ch)
                    def _():
                        held_copy(ch).wait()

            out = jnp.dot(a_bf[...], held[c], preferred_element_type=jnp.float32)
            for h in range(per_chunk):
                p = c * per_chunk + h
                y_out[p] = out[:, h * piece:(h + 1) * piece]
                y_copy(p).start()
            return 0

        lax.fori_loop(0, n_chunks, send_half, 0)
        pl.semaphore_wait(credit_x, 1)
        pl.semaphore_wait(credit_p, 1)
        emis_copy(t, par).wait()

        def pieces(c, out):
            for h in range(per_chunk):
                p = c * per_chunk + h
                y_copy(p).wait_recv()
                cols = pl.ds(pl.multiple_of(p * piece, piece), piece)
                emit_piece(p, out[:, h * piece:(h + 1) * piece] + y_in[p], cols, par)

            @pl.when(c > 0)
            def _():
                for h in range(per_chunk):
                    forward((c - 1) * per_chunk + h)

        def own_held(c, _):
            @pl.when(t == 1)
            def _():
                for ch in range(n_held_own):
                    @pl.when(c == ch)
                    def _():
                        held_copy(n_chunks + ch).wait()

            pieces(c, jnp.dot(a_bf[...], held[n_chunks + c], preferred_element_type=jnp.float32))
            return 0

        lax.fori_loop(0, n_held_own, own_held, 0)

        def own_streamed(c, _):
            out = None
            for k in range(k_parts):
                ring_copy(c, k).wait()
                term = jnp.dot(a_bf[:, k * depth:(k + 1) * depth], ring[k], preferred_element_type=jnp.float32)
                out = term if out is None else out + term
                last = c == n_chunks - 1

                @pl.when(jnp.logical_not(last))
                def _():
                    ring_copy(c + 1, k).start()

                @pl.when(jnp.logical_and(last, t < n_steps - 1))
                def _():
                    ring_copy(n_held_own, k).start()

            pieces(c, out)
            return 0

        lax.fori_loop(n_held_own, n_chunks, own_streamed, 0)
        for p in range(n_pieces):
            y_copy(p).wait_send()
        finish(t, n_pieces - per_chunk)
        return 0

    lax.fori_loop(1, n_steps, one_step, 0)


def run_forward(a_two, emis, init_row, len_pack, len_col, n_steps, rows, width):
    piece, chunk, depth, n_held = 256, 512, 2048, 6
    sources = a_two.shape[1]
    n_pieces = width // piece
    dma = pltpu.SemaphoreType.DMA
    any_spec = pl.BlockSpec(memory_space=pl.ANY)
    vmem = pl.BlockSpec(memory_space=pltpu.VMEM)
    return pl.pallas_call(
        functools.partial(forward_kernel, n_steps, rows, width, piece, chunk, depth),
        out_shape=(jax.ShapeDtypeStruct((GROUP, LANES), jnp.float32), jax.ShapeDtypeStruct((rows, width), jnp.float32)),
        in_specs=[any_spec, any_spec, vmem, vmem, vmem],
        out_specs=(vmem, vmem),
        scratch_shapes=[
            pltpu.VMEM((n_held, sources, chunk), jnp.bfloat16),
            pltpu.VMEM((sources // depth, depth, chunk), jnp.bfloat16),
            pltpu.VMEM((rows, sources), jnp.bfloat16),
            pltpu.VMEM((4, n_pieces, rows, piece), jnp.float32),
            pltpu.VMEM((n_pieces, rows, piece), jnp.float32),
            pltpu.VMEM((n_pieces, rows, piece), jnp.float32),
            pltpu.VMEM((2, rows, width), jnp.bfloat16),
            pltpu.VMEM((2, 8, GROUP, LANES), jnp.float32),
            pltpu.VMEM((rows, LANES), jnp.float32),
            pltpu.VMEM((rows, LANES), jnp.float32),
            dma((n_held,)), dma((sources // depth,)), dma((2,)),
            dma((n_pieces,)), dma((n_pieces,)), dma((n_pieces,)), dma((n_pieces,)),
            dma((n_pieces,)), dma((n_pieces,)), dma((n_pieces,)), dma((n_pieces,)),
            dma((8,)), dma((2, 8)),
            pltpu.SemaphoreType.REGULAR, pltpu.SemaphoreType.REGULAR,
        ],
        compiler_params=pltpu.CompilerParams(collective_id=0, has_side_effects=True, vmem_limit_bytes=67000000),
    )(a_two, emis, init_row, len_pack, len_col)


def solution(mesh):
    vec_axes = ('rows', 'states')

    def local_forward(trans_blk, emit_blk, init_blk, tokens, lengths):
        batch, n_steps = tokens.shape
        width = init_blk.shape[0]
        a_two = jnp.transpose(trans_blk, (1, 0, 2))
        flat = tokens.T.reshape(-1)
        emis = emit_blk.T.at[flat].get(mode='promise_in_bounds').reshape(n_steps, batch, width)
        len_pack = jnp.pad(lengths.reshape(batch // GROUP, GROUP).T, ((0, 0), (0, LANES - batch // GROUP)))
        len_col = jnp.broadcast_to(lengths[:, None], (batch, LANES))
        ll, alpha = run_forward(a_two, emis, init_blk[None, :], len_pack, len_col, n_steps, batch, width)
        return ll[:, :batch // GROUP].T.reshape(batch), alpha

    return jax.shard_map(local_forward, mesh=mesh, in_specs=(P('rows', None, 'states'), P(vec_axes, None), P(vec_axes), P('seqs', None), P('seqs')), out_specs=(P('seqs'), P('seqs', vec_axes)), check_vma=False)
```

```python
import functools

import jax
import jax.numpy as jnp
from jax import lax
from jax.experimental import pallas as pl
from jax.experimental.pallas import tpu as pltpu
from jax.sharding import PartitionSpec as P

MESH = pl.DeviceIdType.MESH
LANES = 128
GROUP = 8


def forward_kernel(
    n_steps, rows, width, piece, chunk, depth,
    a_hbm, emis_hbm, init_ref, end_pack, end_col,
    ll_ref, alpha_ref,
    held, ring, a_bf, gath, y_out, y_in, emis, c_buf, c_acc, inv_b,
    held_sem, ring_sem, emis_sem, y_ss, y_rs, x_ss, x_rs, p_ss, p_rs, f_ss, f_rs, c_ss, c_rs,
    credit_x, credit_p,
):
    n_pieces = width // piece
    n_chunks = width // chunk
    n_held_own = held.shape[0] - n_chunks
    per_chunk = chunk // piece
    k_parts = a_bf.shape[1] // depth
    row = lax.axis_index('rows')
    st = lax.axis_index('states')
    across = lax.rem(st + 2, 4)
    partner = st + 1 - 2 * lax.rem(st, 2)
    other = 1 - row
    me = row * 4 + st
    to_y = {'rows': other}
    to_x = {'states': across}
    to_p = {'states': partner}
    peers = []
    for k in range(1, 8):
        peers.append({'rows': lax.rem(row + k // 4, 2), 'states': lax.rem(st + k % 4, 4)})

    barrier = pltpu.get_barrier_semaphore()
    for peer in peers:
        pl.semaphore_signal(barrier, inc=1, device_id=peer, device_id_type=MESH)

    def held_copy(ch):
        half, c = (other, ch) if ch < n_chunks else (row, 2 * (ch - n_chunks) + 1)
        return pltpu.make_async_copy(a_hbm.at[half, :, pl.ds(c * chunk, chunk)], held.at[ch], held_sem.at[ch])

    def ring_copy(c, k):
        cols = pl.ds(pl.multiple_of(c * chunk, chunk), chunk)
        return pltpu.make_async_copy(a_hbm.at[row, pl.ds(k * depth, depth), cols], ring.at[k], ring_sem.at[k])

    def emis_copy(t, slot):
        return pltpu.make_async_copy(emis_hbm.at[t, pl.ds(0, rows)], emis.at[slot], emis_sem.at[slot])

    def remote(src, dst, ss, rs, dev):
        return pltpu.make_async_remote_copy(src_ref=src, dst_ref=dst, send_sem=ss, recv_sem=rs, device_id=dev, device_id_type=MESH)

    def y_copy(p):
        return remote(y_out.at[p], y_in.at[p], y_ss.at[p], y_rs.at[p], to_y)

    def x_copy(p):
        return remote(gath.at[st, p], gath.at[st, p], x_ss.at[p], x_rs.at[p], to_x)

    def x_arrived(p):
        return remote(gath.at[across, p], gath.at[across, p], x_ss.at[p], x_rs.at[p], to_x)

    def p_copy(p):
        return remote(gath.at[st, p], gath.at[st, p], p_ss.at[p], p_rs.at[p], to_p)

    def p_arrived(p):
        return remote(gath.at[partner, p], gath.at[partner, p], p_ss.at[p], p_rs.at[p], to_p)

    def f_copy(p):
        return remote(gath.at[across, p], gath.at[across, p], f_ss.at[p], f_rs.at[p], to_p)

    def f_arrived(p):
        far = lax.rem(partner + 2, 4)
        return remote(gath.at[far, p], gath.at[far, p], f_ss.at[p], f_rs.at[p], to_p)

    def c_copy(par, k):
        return remote(c_buf.at[par, me], c_buf.at[par, me], c_ss.at[k], c_rs.at[par, k], peers[k - 1])

    def c_arrived(par, k):
        src = lax.rem(row + k // 4, 2) * 4 + lax.rem(st + 4 - k % 4, 4)
        return remote(c_buf.at[par, src], c_buf.at[par, src], c_ss.at[k], c_rs.at[par, k], peers[k - 1])

    emis_copy(0, 0).start()
    for ch in range(held.shape[0]):
        held_copy(ch).start()
    for k in range(k_parts):
        ring_copy(0, k).start()
    emis_copy(1, 1).start()
    pl.semaphore_wait(barrier, 7)

    lane = lax.broadcasted_iota(jnp.int32, (GROUP, LANES), 1)
    ll_ref[...] = jnp.zeros_like(ll_ref)
    alpha_ref[...] = jnp.zeros_like(alpha_ref)

    def emit_piece(p, value, t, par):
        for j in range(piece // LANES):
            cols = pl.ds(pl.multiple_of(p * piece + j * LANES, LANES), LANES)
            fresh = jnp.broadcast_to(init_ref[:, cols], (rows, LANES))
            if value is not None:
                fresh = jnp.where(t == end_col[0], fresh, value[:, j * LANES:(j + 1) * LANES])
            r = fresh * emis[par, :, cols].astype(jnp.float32)
            gath[st, p, :, j * LANES:(j + 1) * LANES] = r
            c_acc[...] += r
        x_copy(p).start()
        p_copy(p).start()

    def forward(p):
        x_arrived(p).wait_recv()
        f_copy(p).start()

    def finish(t, first_forward):
        par = lax.rem(t, 2)
        pack = jnp.zeros((GROUP, LANES), jnp.float32)
        for i in range(rows // GROUP):
            total = jnp.sum(c_acc[pl.ds(i * GROUP, GROUP), :], axis=1, keepdims=True)
            pack = jnp.where(lane == i, total, pack)
        c_buf[par, me] = pack
        for k in range(1, 8):
            c_copy(par, k).start()
        c_acc[...] = jnp.zeros_like(c_acc)
        for p in range(first_forward, n_pieces):
            forward(p)
        for k in range(1, 8):
            c_arrived(par, k).wait_recv()
        total = c_buf[par, 0]
        for k in range(1, 8):
            total = total + c_buf[par, k]
        log_c = jnp.log(total)
        first = t < end_pack[0]
        ll_ref[0] += jnp.where(first, log_c, 0.0)
        ll_ref[1] += jnp.where(jnp.logical_and(jnp.logical_not(first), t < end_pack[1]), log_c, 0.0)
        inv = 1.0 / total
        for i in range(rows // GROUP):
            inv_b[pl.ds(i * GROUP, GROUP), :] = jnp.broadcast_to(inv[:, i:i + 1], (GROUP, LANES))

        def convert(src, p):
            scale = inv_b[...]
            for j in range(piece // LANES):
                at = pl.multiple_of(src * width + p * piece + j * LANES, LANES)
                a_bf[:, pl.ds(at, LANES)] = (gath[src, p, :, j * LANES:(j + 1) * LANES] * scale).astype(jnp.bfloat16)

        def convert_own(p, _):
            convert(st, p)
            convert(across, p)
            return 0

        lax.fori_loop(0, n_pieces, convert_own, 0)

        def convert_near(p, _):
            p_arrived(p).wait_recv()
            f_arrived(p).wait_recv()
            convert(partner, p)
            convert(lax.rem(partner + 2, 4), p)
            return 0

        lax.fori_loop(0, n_pieces, convert_near, 0)
        for p in range(n_pieces):
            x_copy(p).wait_send()
            p_copy(p).wait_send()
            f_copy(p).wait_send()
        for k in range(1, 8):
            c_copy(par, k).wait_send()

        @pl.when(t < n_steps - 1)
        def _():
            pl.semaphore_signal(credit_x, inc=1, device_id=to_x, device_id_type=MESH)
            pl.semaphore_signal(credit_p, inc=1, device_id=to_p, device_id_type=MESH)

    def capture(t):
        first = t < end_col[0]
        second = jnp.logical_and(jnp.logical_not(first), t < end_col[1])
        scale = inv_b[...]
        for p in range(n_pieces):
            for j in range(piece // LANES):
                cols = pl.ds(p * piece + j * LANES, LANES)
                a = gath[st, p, :, j * LANES:(j + 1) * LANES] * scale
                alpha_ref[0, :, cols] = jnp.where(first, a, alpha_ref[0, :, cols])
                alpha_ref[1, :, cols] = jnp.where(second, a, alpha_ref[1, :, cols])

    c_acc[...] = jnp.zeros_like(c_acc)
    emis_copy(0, 0).wait()
    for p in range(n_pieces):
        emit_piece(p, None, 0, 0)
    finish(0, 0)

    def one_step(t, _):
        par = lax.rem(t, 2)

        @pl.when(t + 1 < n_steps)
        def _():
            emis_copy(t + 1, 1 - par).start()

        def send_half(c, _):
            @pl.when(t == 1)
            def _():
                for ch in range(n_chunks):
                    @pl.when(c == ch)
                    def _():
                        held_copy(ch).wait()

            out = jnp.dot(a_bf[...], held[c], preferred_element_type=jnp.float32)
            for h in range(per_chunk):
                p = c * per_chunk + h
                y_out[p] = out[:, h * piece:(h + 1) * piece]
                y_copy(p).start()
            return 0

        lax.fori_loop(0, n_chunks, send_half, 0)
        capture(t - 1)
        pl.semaphore_wait(credit_x, 1)
        pl.semaphore_wait(credit_p, 1)
        emis_copy(t, par).wait()

        def pieces(c, out):
            for h in range(per_chunk):
                p = c * per_chunk + h
                y_copy(p).wait_recv()
                emit_piece(p, out[:, h * piece:(h + 1) * piece] + y_in[p], t, par)

        def forward_chunk(c):
            for h in range(per_chunk):
                forward(c * per_chunk + h)

        def own_pair(i, _):
            c = 2 * i
            out = None
            for k in range(k_parts):
                ring_copy(c, k).wait()
                term = jnp.dot(a_bf[:, k * depth:(k + 1) * depth], ring[k], preferred_element_type=jnp.float32)
                out = term if out is None else out + term
                last = i == n_held_own - 1

                @pl.when(jnp.logical_not(last))
                def _():
                    ring_copy(c + 2, k).start()

                @pl.when(jnp.logical_and(last, t < n_steps - 1))
                def _():
                    ring_copy(0, k).start()

            pieces(c, out)

            @pl.when(i > 0)
            def _():
                forward_chunk(c - 1)

            @pl.when(t == 1)
            def _():
                for ch in range(n_held_own):
                    @pl.when(i == ch)
                    def _():
                        held_copy(n_chunks + ch).wait()

            pieces(c + 1, jnp.dot(a_bf[...], held[n_chunks + i], preferred_element_type=jnp.float32))
            forward_chunk(c)
            return 0

        lax.fori_loop(0, n_held_own, own_pair, 0)
        for p in range(n_pieces):
            y_copy(p).wait_send()
        finish(t, n_pieces - per_chunk)
        return 0

    lax.fori_loop(1, n_steps, one_step, 0)
    capture(n_steps - 1)


def run_forward(a_two, emis, init_row, end_pack, end_col, call_id):
    n_steps, rows, width = emis.shape
    piece, chunk, depth, n_held = 256, 512, 2048, 6
    sources = a_two.shape[1]
    n_pieces = width // piece
    dma = pltpu.SemaphoreType.DMA
    any_spec = pl.BlockSpec(memory_space=pl.ANY)
    vmem = pl.BlockSpec(memory_space=pltpu.VMEM)
    return pl.pallas_call(
        functools.partial(forward_kernel, n_steps, rows, width, piece, chunk, depth),
        out_shape=(jax.ShapeDtypeStruct((2, GROUP, LANES), jnp.float32), jax.ShapeDtypeStruct((2, rows, width), jnp.float32)),
        in_specs=[any_spec, any_spec, vmem, vmem, vmem],
        out_specs=(vmem, vmem),
        scratch_shapes=[
            pltpu.VMEM((n_held, sources, chunk), jnp.bfloat16),
            pltpu.VMEM((sources // depth, depth, chunk), jnp.bfloat16),
            pltpu.VMEM((rows, sources), jnp.bfloat16),
            pltpu.VMEM((4, n_pieces, rows, piece), jnp.float32),
            pltpu.VMEM((n_pieces, rows, piece), jnp.float32),
            pltpu.VMEM((n_pieces, rows, piece), jnp.float32),
            pltpu.VMEM((2, rows, width), jnp.bfloat16),
            pltpu.VMEM((2, 8, GROUP, LANES), jnp.float32),
            pltpu.VMEM((rows, LANES), jnp.float32),
            pltpu.VMEM((rows, LANES), jnp.float32),
            dma((n_held,)), dma((sources // depth,)), dma((2,)),
            dma((n_pieces,)), dma((n_pieces,)), dma((n_pieces,)), dma((n_pieces,)),
            dma((n_pieces,)), dma((n_pieces,)), dma((n_pieces,)), dma((n_pieces,)),
            dma((8,)), dma((2, 8)),
            pltpu.SemaphoreType.REGULAR, pltpu.SemaphoreType.REGULAR,
        ],
        compiler_params=pltpu.CompilerParams(collective_id=call_id, has_side_effects=True, vmem_limit_bytes=67000000),
    )(a_two, emis, init_row, end_pack, end_col)


def second_of(ranked, rows):
    batch = ranked.shape[0]
    alone = 2 * rows - batch
    return jnp.concatenate([jnp.zeros((alone,) + ranked.shape[1:], ranked.dtype), ranked[rows:][::-1]])


def solution(mesh):
    vec_axes = ('rows', 'states')

    def local_forward(trans_blk, emit_blk, init_blk, tokens, lengths):
        batch, n_steps = tokens.shape
        width = init_blk.shape[0]
        a_two = jnp.transpose(trans_blk, (1, 0, 2))
        table = emit_blk.T
        seq = jnp.arange(batch)
        longer = (lengths[None, :] > lengths[:, None]) | ((lengths[None, :] == lengths[:, None]) & (seq[None, :] < seq[:, None]))
        rank = jnp.sum(longer.astype(jnp.int32), axis=1)
        at_rank = rank[None, :] == seq[:, None]
        len_ranked = jnp.sum(jnp.where(at_rank, lengths[None, :], 0), axis=1)
        tok_ranked = jnp.sum(jnp.where(at_rank[:, :, None], tokens[None, :, :], 0), axis=1)

        def run(rows, call_id):
            def branch(a_two, table, init_blk, rank, len_ranked, tok_ranked):
                end_1 = len_ranked[:rows]
                end_2 = end_1 + second_of(len_ranked, rows)
                step = jnp.arange(n_steps)
                since = step[:, None] - end_1[None, :]
                later = jnp.sum(jnp.where(since[:, :, None] == step[None, None, :], second_of(tok_ranked, rows)[None, :, :], 0), axis=2)
                tok = jnp.where(since < 0, tok_ranked[:rows].T, later)
                emis = table.at[tok.reshape(-1)].get(mode='promise_in_bounds').reshape(n_steps, rows, width)
                ends = jnp.stack([end_1, end_2])
                packed = jnp.swapaxes(ends.reshape(2, rows // GROUP, GROUP), 1, 2)
                end_pack = jnp.pad(packed, ((0, 0), (0, 0), (0, LANES - rows // GROUP)))
                end_col = jnp.broadcast_to(ends[:, :, None], (2, rows, LANES))
                ll, alpha = run_forward(a_two, emis, init_blk[None, :], end_pack, end_col, call_id)
                at = jnp.where(rank < rows, rank, 3 * rows - 1 - rank)
                ll_rows = jnp.swapaxes(ll[:, :, :rows // GROUP], 1, 2).reshape(2 * rows)
                loglik = jnp.sum(jnp.where(at[:, None] == jnp.arange(2 * rows)[None, :], ll_rows[None, :], 0.0), axis=1)
                return loglik, alpha.reshape(2 * rows, width).at[at].get(mode='promise_in_bounds')

            return branch

        def fits(rows):
            return jnp.max(jnp.where(jnp.arange(rows) >= 2 * rows - batch, len_ranked[:rows] + second_of(len_ranked, rows), 0)) <= n_steps

        sizes = (40, 48, batch)
        pick = jnp.where(fits(40), 0, jnp.where(fits(48), 1, 2))
        return lax.switch(pick, [run(m, k) for k, m in enumerate(sizes)], a_two, table, init_blk, rank, len_ranked, tok_ranked)

    return jax.shard_map(local_forward, mesh=mesh, in_specs=(P('rows', None, 'states'), P(vec_axes, None), P(vec_axes), P('seqs', None), P('seqs')), out_specs=(P('seqs'), P('seqs', vec_axes)), check_vma=False)
```

```python
import functools

import jax
import jax.numpy as jnp
from jax import lax
from jax.experimental import pallas as pl
from jax.experimental.pallas import tpu as pltpu
from jax.sharding import PartitionSpec as P

MESH = pl.DeviceIdType.MESH
LANES = 128
GROUP = 8


def forward_kernel(
    n_steps, rows, width, piece, chunk, depth,
    a_hbm, emis_hbm, init_ref, end_pack, end_col,
    ll_ref, alpha_ref,
    held, ring, a_bf, gath, y_out, y_in, emis, c_buf, c_acc, inv_b,
    held_sem, ring_sem, emis_sem, y_ss, y_rs, x_ss, x_rs, p_ss, p_rs, f_ss, f_rs, c_ss, c_rs,
    credit_x, credit_p,
):
    n_pieces = width // piece
    n_chunks = width // chunk
    n_held_own = held.shape[0] - n_chunks
    per_chunk = chunk // piece
    k_parts = a_bf.shape[1] // depth
    row = lax.axis_index('rows')
    st = lax.axis_index('states')
    across = lax.rem(st + 2, 4)
    partner = st + 1 - 2 * lax.rem(st, 2)
    other = 1 - row
    me = row * 4 + st
    to_y = {'rows': other}
    to_x = {'states': across}
    to_p = {'states': partner}
    peers = []
    for k in range(1, 8):
        peers.append({'rows': lax.rem(row + k // 4, 2), 'states': lax.rem(st + k % 4, 4)})

    barrier = pltpu.get_barrier_semaphore()
    for peer in peers:
        pl.semaphore_signal(barrier, inc=1, device_id=peer, device_id_type=MESH)

    def held_copy(ch):
        half, c = (other, ch) if ch < n_chunks else (row, 2 * (ch - n_chunks) + 1)
        return pltpu.make_async_copy(a_hbm.at[half, :, pl.ds(c * chunk, chunk)], held.at[ch], held_sem.at[ch])

    def ring_copy(c, k):
        cols = pl.ds(pl.multiple_of(c * chunk, chunk), chunk)
        return pltpu.make_async_copy(a_hbm.at[row, pl.ds(k * depth, depth), cols], ring.at[k], ring_sem.at[k])

    def emis_copy(t, slot):
        return pltpu.make_async_copy(emis_hbm.at[t, pl.ds(0, rows)], emis.at[slot], emis_sem.at[slot])

    def remote(src, dst, ss, rs, dev):
        return pltpu.make_async_remote_copy(src_ref=src, dst_ref=dst, send_sem=ss, recv_sem=rs, device_id=dev, device_id_type=MESH)

    def y_copy(p):
        return remote(y_out.at[p], y_in.at[p], y_ss.at[p], y_rs.at[p], to_y)

    def x_copy(p):
        return remote(gath.at[st, p], gath.at[st, p], x_ss.at[p], x_rs.at[p], to_x)

    def x_arrived(p):
        return remote(gath.at[across, p], gath.at[across, p], x_ss.at[p], x_rs.at[p], to_x)

    def p_copy(p):
        return remote(gath.at[st, p], gath.at[st, p], p_ss.at[p], p_rs.at[p], to_p)

    def p_arrived(p):
        return remote(gath.at[partner, p], gath.at[partner, p], p_ss.at[p], p_rs.at[p], to_p)

    def f_copy(p):
        return remote(gath.at[across, p], gath.at[across, p], f_ss.at[p], f_rs.at[p], to_p)

    def f_arrived(p):
        far = lax.rem(partner + 2, 4)
        return remote(gath.at[far, p], gath.at[far, p], f_ss.at[p], f_rs.at[p], to_p)

    def c_copy(par, k):
        return remote(c_buf.at[par, me], c_buf.at[par, me], c_ss.at[k], c_rs.at[par, k], peers[k - 1])

    def c_arrived(par, k):
        src = lax.rem(row + k // 4, 2) * 4 + lax.rem(st + 4 - k % 4, 4)
        return remote(c_buf.at[par, src], c_buf.at[par, src], c_ss.at[k], c_rs.at[par, k], peers[k - 1])

    emis_copy(0, 0).start()
    for ch in range(held.shape[0]):
        held_copy(ch).start()
    for k in range(k_parts):
        ring_copy(0, k).start()
    emis_copy(1, 1).start()
    pl.semaphore_wait(barrier, 7)

    lane = lax.broadcasted_iota(jnp.int32, (GROUP, LANES), 1)
    ll_ref[...] = jnp.zeros_like(ll_ref)
    alpha_ref[...] = jnp.zeros_like(alpha_ref)

    def emit_piece(p, value, t, par):
        for j in range(piece // LANES):
            cols = pl.ds(pl.multiple_of(p * piece + j * LANES, LANES), LANES)
            fresh = jnp.broadcast_to(init_ref[:, cols], (rows, LANES))
            if value is not None:
                fresh = jnp.where(t == end_col[0], fresh, value[:, j * LANES:(j + 1) * LANES])
            r = fresh * emis[par, :, cols].astype(jnp.float32)
            gath[st, p, :, j * LANES:(j + 1) * LANES] = r
            c_acc[...] += r
        x_copy(p).start()
        p_copy(p).start()

    def forward(p):
        x_arrived(p).wait_recv()
        f_copy(p).start()

    def finish(t):
        par = lax.rem(t, 2)
        pack = jnp.zeros((GROUP, LANES), jnp.float32)
        for i in range(rows // GROUP):
            total = jnp.sum(c_acc[pl.ds(i * GROUP, GROUP), :], axis=1, keepdims=True)
            pack = jnp.where(lane == i, total, pack)
        c_buf[par, me] = pack
        for k in range(1, 8):
            c_copy(par, k).start()
        c_acc[...] = jnp.zeros_like(c_acc)
        for p in range(n_pieces):
            forward(p)
        for k in range(1, 8):
            c_arrived(par, k).wait_recv()
        total = c_buf[par, 0]
        for k in range(1, 8):
            total = total + c_buf[par, k]
        log_c = jnp.log(total)
        first = t < end_pack[0]
        ll_ref[0] += jnp.where(first, log_c, 0.0)
        ll_ref[1] += jnp.where(jnp.logical_and(jnp.logical_not(first), t < end_pack[1]), log_c, 0.0)
        inv = 1.0 / total
        for i in range(rows // GROUP):
            inv_b[pl.ds(i * GROUP, GROUP), :] = jnp.broadcast_to(inv[:, i:i + 1], (GROUP, LANES))

        def convert(src, p):
            scale = inv_b[...]
            for j in range(piece // LANES):
                at = pl.multiple_of(src * width + p * piece + j * LANES, LANES)
                a_bf[:, pl.ds(at, LANES)] = (gath[src, p, :, j * LANES:(j + 1) * LANES] * scale).astype(jnp.bfloat16)

        def convert_own(p, _):
            convert(st, p)
            convert(across, p)
            return 0

        lax.fori_loop(0, n_pieces, convert_own, 0)

        def convert_near(p, _):
            p_arrived(p).wait_recv()
            f_arrived(p).wait_recv()
            convert(partner, p)
            convert(lax.rem(partner + 2, 4), p)
            return 0

        lax.fori_loop(0, n_pieces, convert_near, 0)
        for p in range(n_pieces):
            x_copy(p).wait_send()
            p_copy(p).wait_send()
            f_copy(p).wait_send()
        for k in range(1, 8):
            c_copy(par, k).wait_send()

        @pl.when(t < n_steps - 1)
        def _():
            pl.semaphore_signal(credit_x, inc=1, device_id=to_x, device_id_type=MESH)
            pl.semaphore_signal(credit_p, inc=1, device_id=to_p, device_id_type=MESH)

    def capture(t):
        first = t < end_col[0]
        second = jnp.logical_and(jnp.logical_not(first), t < end_col[1])
        scale = inv_b[...]
        for p in range(n_pieces):
            for j in range(piece // LANES):
                cols = pl.ds(p * piece + j * LANES, LANES)
                a = gath[st, p, :, j * LANES:(j + 1) * LANES] * scale
                alpha_ref[0, :, cols] = jnp.where(first, a, alpha_ref[0, :, cols])
                alpha_ref[1, :, cols] = jnp.where(second, a, alpha_ref[1, :, cols])

    c_acc[...] = jnp.zeros_like(c_acc)
    emis_copy(0, 0).wait()
    for p in range(n_pieces):
        emit_piece(p, None, 0, 0)
    finish(0)

    def one_step(t, _):
        par = lax.rem(t, 2)

        @pl.when(t + 1 < n_steps)
        def _():
            emis_copy(t + 1, 1 - par).start()

        def send_half(c, _):
            @pl.when(t == 1)
            def _():
                for ch in range(n_chunks):
                    @pl.when(c == ch)
                    def _():
                        held_copy(ch).wait()

            out = jnp.dot(a_bf[...], held[c], preferred_element_type=jnp.float32)
            for h in range(per_chunk):
                p = c * per_chunk + h
                y_out[p] = out[:, h * piece:(h + 1) * piece]
                y_copy(p).start()
            return 0

        lax.fori_loop(0, n_chunks, send_half, 0)
        capture(t - 1)
        pl.semaphore_wait(credit_x, 1)
        pl.semaphore_wait(credit_p, 1)
        emis_copy(t, par).wait()

        def pieces(c, out):
            for h in range(per_chunk):
                p = c * per_chunk + h
                y_copy(p).wait_recv()
                emit_piece(p, out[:, h * piece:(h + 1) * piece] + y_in[p], t, par)

        def own_pair(i, _):
            c = 2 * i
            out = None
            for k in range(k_parts):
                ring_copy(c, k).wait()
                term = jnp.dot(a_bf[:, k * depth:(k + 1) * depth], ring[k], preferred_element_type=jnp.float32)
                out = term if out is None else out + term
                last = i == n_held_own - 1

                @pl.when(jnp.logical_not(last))
                def _():
                    ring_copy(c + 2, k).start()

                @pl.when(jnp.logical_and(last, t < n_steps - 1))
                def _():
                    ring_copy(0, k).start()

            pieces(c, out)

            @pl.when(t == 1)
            def _():
                for ch in range(n_held_own):
                    @pl.when(i == ch)
                    def _():
                        held_copy(n_chunks + ch).wait()

            pieces(c + 1, jnp.dot(a_bf[...], held[n_chunks + i], preferred_element_type=jnp.float32))
            return 0

        lax.fori_loop(0, n_held_own, own_pair, 0)
        for p in range(n_pieces):
            y_copy(p).wait_send()
        finish(t)
        return 0

    lax.fori_loop(1, n_steps, one_step, 0)
    capture(n_steps - 1)


def run_forward(a_two, emis, init_row, end_pack, end_col, call_id):
    n_steps, rows, width = emis.shape
    piece, chunk, depth, n_held = 256, 512, 2048, 6
    sources = a_two.shape[1]
    n_pieces = width // piece
    dma = pltpu.SemaphoreType.DMA
    any_spec = pl.BlockSpec(memory_space=pl.ANY)
    vmem = pl.BlockSpec(memory_space=pltpu.VMEM)
    return pl.pallas_call(
        functools.partial(forward_kernel, n_steps, rows, width, piece, chunk, depth),
        out_shape=(jax.ShapeDtypeStruct((2, GROUP, LANES), jnp.float32), jax.ShapeDtypeStruct((2, rows, width), jnp.float32)),
        in_specs=[any_spec, any_spec, vmem, vmem, vmem],
        out_specs=(vmem, vmem),
        scratch_shapes=[
            pltpu.VMEM((n_held, sources, chunk), jnp.bfloat16),
            pltpu.VMEM((sources // depth, depth, chunk), jnp.bfloat16),
            pltpu.VMEM((rows, sources), jnp.bfloat16),
            pltpu.VMEM((4, n_pieces, rows, piece), jnp.float32),
            pltpu.VMEM((n_pieces, rows, piece), jnp.float32),
            pltpu.VMEM((n_pieces, rows, piece), jnp.float32),
            pltpu.VMEM((2, rows, width), jnp.bfloat16),
            pltpu.VMEM((2, 8, GROUP, LANES), jnp.float32),
            pltpu.VMEM((rows, LANES), jnp.float32),
            pltpu.VMEM((rows, LANES), jnp.float32),
            dma((n_held,)), dma((sources // depth,)), dma((2,)),
            dma((n_pieces,)), dma((n_pieces,)), dma((n_pieces,)), dma((n_pieces,)),
            dma((n_pieces,)), dma((n_pieces,)), dma((n_pieces,)), dma((n_pieces,)),
            dma((8,)), dma((2, 8)),
            pltpu.SemaphoreType.REGULAR, pltpu.SemaphoreType.REGULAR,
        ],
        compiler_params=pltpu.CompilerParams(collective_id=call_id, has_side_effects=True, vmem_limit_bytes=67000000),
    )(a_two, emis, init_row, end_pack, end_col)


def second_of(ranked, rows):
    batch = ranked.shape[0]
    alone = 2 * rows - batch
    return jnp.concatenate([jnp.zeros((alone,) + ranked.shape[1:], ranked.dtype), ranked[rows:][::-1]])


def solution(mesh):
    vec_axes = ('rows', 'states')

    def local_forward(trans_blk, emit_blk, init_blk, tokens, lengths):
        batch, n_steps = tokens.shape
        width = init_blk.shape[0]
        a_two = jnp.transpose(trans_blk, (1, 0, 2))
        table = emit_blk.T
        seq = jnp.arange(batch)
        longer = (lengths[None, :] > lengths[:, None]) | ((lengths[None, :] == lengths[:, None]) & (seq[None, :] < seq[:, None]))
        rank = jnp.sum(longer.astype(jnp.int32), axis=1)
        at_rank = rank[None, :] == seq[:, None]
        len_ranked = jnp.sum(jnp.where(at_rank, lengths[None, :], 0), axis=1)
        tok_ranked = jnp.sum(jnp.where(at_rank[:, :, None], tokens[None, :, :], 0), axis=1)

        def run(rows, call_id):
            def branch(a_two, table, init_blk, rank, len_ranked, tok_ranked):
                end_1 = len_ranked[:rows]
                end_2 = end_1 + second_of(len_ranked, rows)
                step = jnp.arange(n_steps)
                since = step[:, None] - end_1[None, :]
                later = jnp.sum(jnp.where(since[:, :, None] == step[None, None, :], second_of(tok_ranked, rows)[None, :, :], 0), axis=2)
                tok = jnp.where(since < 0, tok_ranked[:rows].T, later)
                emis = table.at[tok.reshape(-1)].get(mode='promise_in_bounds').reshape(n_steps, rows, width)
                ends = jnp.stack([end_1, end_2])
                packed = jnp.swapaxes(ends.reshape(2, rows // GROUP, GROUP), 1, 2)
                end_pack = jnp.pad(packed, ((0, 0), (0, 0), (0, LANES - rows // GROUP)))
                end_col = jnp.broadcast_to(ends[:, :, None], (2, rows, LANES))
                ll, alpha = run_forward(a_two, emis, init_blk[None, :], end_pack, end_col, call_id)
                at = jnp.where(rank < rows, rank, 3 * rows - 1 - rank)
                ll_rows = jnp.swapaxes(ll[:, :, :rows // GROUP], 1, 2).reshape(2 * rows)
                loglik = jnp.sum(jnp.where(at[:, None] == jnp.arange(2 * rows)[None, :], ll_rows[None, :], 0.0), axis=1)
                return loglik, alpha.reshape(2 * rows, width).at[at].get(mode='promise_in_bounds')

            return branch

        def fits(rows):
            return jnp.max(jnp.where(jnp.arange(rows) >= 2 * rows - batch, len_ranked[:rows] + second_of(len_ranked, rows), 0)) <= n_steps

        sizes = (40, 48, batch)
        pick = jnp.where(fits(40), 0, jnp.where(fits(48), 1, 2))
        return lax.switch(pick, [run(m, k) for k, m in enumerate(sizes)], a_two, table, init_blk, rank, len_ranked, tok_ranked)

    return jax.shard_map(local_forward, mesh=mesh, in_specs=(P('rows', None, 'states'), P(vec_axes, None), P(vec_axes), P('seqs', None), P('seqs')), out_specs=(P('seqs'), P('seqs', vec_axes)), check_vma=False)
```

```python
import functools

import jax
import jax.numpy as jnp
from jax import lax
from jax.experimental import pallas as pl
from jax.experimental.pallas import tpu as pltpu
from jax.sharding import PartitionSpec as P

MESH = pl.DeviceIdType.MESH
LANES = 128
GROUP = 8


def forward_kernel(
    n_steps, rows, width, piece, chunk, depth,
    a_hbm, emis_hbm, init_ref, end_pack, end_col,
    ll_ref, alpha_ref,
    held, ring, a_bf, gath, y_out, y_in, emis, c_buf, c_acc, inv_b,
    held_sem, ring_sem, emis_sem, y_ss, y_rs, x_ss, x_rs, p_ss, p_rs, f_ss, f_rs, c_ss, c_rs,
    credit_x, credit_p,
):
    n_pieces = width // piece
    n_chunks = width // chunk
    n_held_own = held.shape[0] - n_chunks
    per_chunk = chunk // piece
    k_parts = a_bf.shape[1] // depth
    row = lax.axis_index('rows')
    st = lax.axis_index('states')
    across = lax.rem(st + 2, 4)
    partner = st + 1 - 2 * lax.rem(st, 2)
    other = 1 - row
    me = row * 4 + st
    to_y = {'rows': other}
    to_x = {'states': across}
    to_p = {'states': partner}
    peers = []
    for k in range(1, 8):
        peers.append({'rows': lax.rem(row + k // 4, 2), 'states': lax.rem(st + k % 4, 4)})

    barrier = pltpu.get_barrier_semaphore()
    for peer in peers:
        pl.semaphore_signal(barrier, inc=1, device_id=peer, device_id_type=MESH)

    def held_copy(ch):
        half, c = (other, ch) if ch < n_chunks else (row, 2 * (ch - n_chunks) + 1)
        return pltpu.make_async_copy(a_hbm.at[half, :, pl.ds(c * chunk, chunk)], held.at[ch], held_sem.at[ch])

    def ring_copy(c, k):
        cols = pl.ds(pl.multiple_of(c * chunk, chunk), chunk)
        return pltpu.make_async_copy(a_hbm.at[row, pl.ds(k * depth, depth), cols], ring.at[k], ring_sem.at[k])

    def emis_copy(t, slot):
        return pltpu.make_async_copy(emis_hbm.at[t, pl.ds(0, rows)], emis.at[slot], emis_sem.at[slot])

    def remote(src, dst, ss, rs, dev):
        return pltpu.make_async_remote_copy(src_ref=src, dst_ref=dst, send_sem=ss, recv_sem=rs, device_id=dev, device_id_type=MESH)

    def y_copy(p):
        return remote(y_out.at[p], y_in.at[p], y_ss.at[p], y_rs.at[p], to_y)

    def own_slot(par):
        return st + par * (4 - st)

    def x_copy(p, par):
        return remote(gath.at[own_slot(par), p], gath.at[st, p], x_ss.at[p], x_rs.at[p], to_x)

    def x_arrived(p):
        return remote(gath.at[across, p], gath.at[across, p], x_ss.at[p], x_rs.at[p], to_x)

    def p_copy(p, par):
        return remote(gath.at[own_slot(par), p], gath.at[st, p], p_ss.at[p], p_rs.at[p], to_p)

    def p_arrived(p):
        return remote(gath.at[partner, p], gath.at[partner, p], p_ss.at[p], p_rs.at[p], to_p)

    def f_copy(p):
        return remote(gath.at[across, p], gath.at[across, p], f_ss.at[p], f_rs.at[p], to_p)

    def f_arrived(p):
        far = lax.rem(partner + 2, 4)
        return remote(gath.at[far, p], gath.at[far, p], f_ss.at[p], f_rs.at[p], to_p)

    def c_copy(par, k):
        return remote(c_buf.at[par, me], c_buf.at[par, me], c_ss.at[k], c_rs.at[par, k], peers[k - 1])

    def c_arrived(par, k):
        src = lax.rem(row + k // 4, 2) * 4 + lax.rem(st + 4 - k % 4, 4)
        return remote(c_buf.at[par, src], c_buf.at[par, src], c_ss.at[k], c_rs.at[par, k], peers[k - 1])

    emis_copy(0, 0).start()
    for ch in range(held.shape[0]):
        held_copy(ch).start()
    for k in range(k_parts):
        ring_copy(0, k).start()
    emis_copy(1, 1).start()
    pl.semaphore_wait(barrier, 7)

    lane = lax.broadcasted_iota(jnp.int32, (GROUP, LANES), 1)
    ll_ref[...] = jnp.zeros_like(ll_ref)
    alpha_ref[...] = jnp.zeros_like(alpha_ref)

    def emit_piece(p, value, t, par):
        for j in range(piece // LANES):
            cols = pl.ds(pl.multiple_of(p * piece + j * LANES, LANES), LANES)
            fresh = jnp.broadcast_to(init_ref[:, cols], (rows, LANES))
            if value is not None:
                fresh = jnp.where(t == end_col[0], fresh, value[:, j * LANES:(j + 1) * LANES])
            r = fresh * emis[par, :, cols].astype(jnp.float32)
            gath[own_slot(par), p, :, j * LANES:(j + 1) * LANES] = r
            c_acc[...] += r
        x_copy(p, par).start()
        p_copy(p, par).start()

    def forward(p):
        x_arrived(p).wait_recv()
        f_copy(p).start()

    def capture(t):
        first = t < end_col[0]
        second = jnp.logical_and(jnp.logical_not(first), t < end_col[1])
        scale = inv_b[...]
        for p in range(n_pieces):
            for j in range(piece // LANES):
                cols = pl.ds(p * piece + j * LANES, LANES)
                a = gath[own_slot(lax.rem(t, 2)), p, :, j * LANES:(j + 1) * LANES] * scale
                alpha_ref[0, :, cols] = jnp.where(first, a, alpha_ref[0, :, cols])
                if alpha_ref.shape[0] > 1:
                    alpha_ref[1, :, cols] = jnp.where(second, a, alpha_ref[1, :, cols])

    def finish(t):
        par = lax.rem(t, 2)
        pack = jnp.zeros((GROUP, LANES), jnp.float32)
        for i in range(rows // GROUP):
            total = jnp.sum(c_acc[pl.ds(i * GROUP, GROUP), :], axis=1, keepdims=True)
            pack = jnp.where(lane == i, total, pack)
        c_buf[par, me] = pack
        for k in range(1, 8):
            c_copy(par, k).start()
        c_acc[...] = jnp.zeros_like(c_acc)
        if not isinstance(t, int):
            capture(t - 1)
        for p in range(n_pieces):
            forward(p)
        for k in range(1, 8):
            c_arrived(par, k).wait_recv()
        total = c_buf[par, 0]
        for k in range(1, 8):
            total = total + c_buf[par, k]
        log_c = jnp.log(total)
        first = t < end_pack[0]
        ll_ref[0] += jnp.where(first, log_c, 0.0)
        ll_ref[1] += jnp.where(jnp.logical_and(jnp.logical_not(first), t < end_pack[1]), log_c, 0.0)
        inv = 1.0 / total
        for i in range(rows // GROUP):
            inv_b[pl.ds(i * GROUP, GROUP), :] = jnp.broadcast_to(inv[:, i:i + 1], (GROUP, LANES))

        def convert(slot, src, p):
            scale = inv_b[...]
            for j in range(piece // LANES):
                at = pl.multiple_of(src * width + p * piece + j * LANES, LANES)
                a_bf[0:rows, pl.ds(at, LANES)] = (gath[slot, p, :, j * LANES:(j + 1) * LANES] * scale).astype(jnp.bfloat16)

        def convert_own(p, _):
            convert(own_slot(par), st, p)
            convert(across, across, p)
            return 0

        lax.fori_loop(0, n_pieces, convert_own, 0)

        def convert_near(p, _):
            p_arrived(p).wait_recv()
            f_arrived(p).wait_recv()
            convert(partner, partner, p)
            far = lax.rem(partner + 2, 4)
            convert(far, far, p)
            return 0

        lax.fori_loop(0, n_pieces, convert_near, 0)
        for p in range(n_pieces):
            x_copy(p, par).wait_send()
            p_copy(p, par).wait_send()
            f_copy(p).wait_send()
        for k in range(1, 8):
            c_copy(par, k).wait_send()

        @pl.when(t < n_steps - 1)
        def _():
            pl.semaphore_signal(credit_x, inc=1, device_id=to_x, device_id_type=MESH)
            pl.semaphore_signal(credit_p, inc=1, device_id=to_p, device_id_type=MESH)

    if a_bf.shape[0] > rows:
        a_bf[rows:, :] = jnp.zeros((a_bf.shape[0] - rows, a_bf.shape[1]), jnp.bfloat16)
    c_acc[...] = jnp.zeros_like(c_acc)
    emis_copy(0, 0).wait()
    for p in range(n_pieces):
        emit_piece(p, None, 0, 0)
    finish(0)

    def one_step(t, _):
        par = lax.rem(t, 2)

        @pl.when(t + 1 < n_steps)
        def _():
            emis_copy(t + 1, 1 - par).start()

        def send_half(c, _):
            @pl.when(t == 1)
            def _():
                for ch in range(n_chunks):
                    @pl.when(c == ch)
                    def _():
                        held_copy(ch).wait()

            out = jnp.dot(a_bf[...], held[c], preferred_element_type=jnp.float32)[0:rows]
            for h in range(per_chunk):
                p = c * per_chunk + h
                y_out[p] = out[:, h * piece:(h + 1) * piece]
                y_copy(p).start()
            return 0

        lax.fori_loop(0, n_held_own, send_half, 0)
        pl.semaphore_wait(credit_x, 1)
        pl.semaphore_wait(credit_p, 1)
        emis_copy(t, par).wait()

        def pieces(c, out):
            for h in range(per_chunk):
                p = c * per_chunk + h
                y_copy(p).wait_recv()
                emit_piece(p, out[:, h * piece:(h + 1) * piece] + y_in[p], t, par)

        def own_pair(i, _):
            c = 2 * i
            lax.fori_loop(2 + 2 * i, 3 + i, send_half, 0)
            out = None
            for k in range(k_parts):
                ring_copy(c, k).wait()
                term = jnp.dot(a_bf[:, k * depth:(k + 1) * depth], ring[k], preferred_element_type=jnp.float32)[0:rows]
                out = term if out is None else out + term
                last = i == n_held_own - 1

                @pl.when(jnp.logical_not(last))
                def _():
                    ring_copy(c + 2, k).start()

                @pl.when(jnp.logical_and(last, t < n_steps - 1))
                def _():
                    ring_copy(0, k).start()

            pieces(c, out)
            lax.fori_loop(3 + i, n_chunks, send_half, 0)

            @pl.when(t == 1)
            def _():
                for ch in range(n_held_own):
                    @pl.when(i == ch)
                    def _():
                        held_copy(n_chunks + ch).wait()

            pieces(c + 1, jnp.dot(a_bf[...], held[n_chunks + i], preferred_element_type=jnp.float32)[0:rows])
            return 0

        lax.fori_loop(0, n_held_own, own_pair, 0)
        for p in range(n_pieces):
            y_copy(p).wait_send()
        finish(t)
        return 0

    lax.fori_loop(1, n_steps, one_step, 0)
    capture(n_steps - 1)


def run_forward(a_two, emis, init_row, end_pack, end_col, n_seqs, call_id):
    n_steps, rows, width = emis.shape
    piece, chunk, depth, n_held = 256, 512, 2048, 6
    sources = a_two.shape[1]
    n_pieces = width // piece
    dma = pltpu.SemaphoreType.DMA
    any_spec = pl.BlockSpec(memory_space=pl.ANY)
    vmem = pl.BlockSpec(memory_space=pltpu.VMEM)
    return pl.pallas_call(
        functools.partial(forward_kernel, n_steps, rows, width, piece, chunk, depth),
        out_shape=(jax.ShapeDtypeStruct((2, GROUP, LANES), jnp.float32), jax.ShapeDtypeStruct((n_seqs, rows, width), jnp.float32)),
        in_specs=[any_spec, any_spec, vmem, vmem, vmem],
        out_specs=(vmem, vmem),
        scratch_shapes=[
            pltpu.VMEM((n_held, sources, chunk), jnp.bfloat16),
            pltpu.VMEM((sources // depth, depth, chunk), jnp.bfloat16),
            pltpu.VMEM((128 if rows <= 48 else rows, sources), jnp.bfloat16),
            pltpu.VMEM((5, n_pieces, rows, piece), jnp.float32),
            pltpu.VMEM((n_pieces, rows, piece), jnp.float32),
            pltpu.VMEM((n_pieces, rows, piece), jnp.float32),
            pltpu.VMEM((2, rows, width), jnp.bfloat16),
            pltpu.VMEM((2, 8, GROUP, LANES), jnp.float32),
            pltpu.VMEM((rows, LANES), jnp.float32),
            pltpu.VMEM((rows, LANES), jnp.float32),
            dma((n_held,)), dma((sources // depth,)), dma((2,)),
            dma((n_pieces,)), dma((n_pieces,)), dma((n_pieces,)), dma((n_pieces,)),
            dma((n_pieces,)), dma((n_pieces,)), dma((n_pieces,)), dma((n_pieces,)),
            dma((8,)), dma((2, 8)),
            pltpu.SemaphoreType.REGULAR, pltpu.SemaphoreType.REGULAR,
        ],
        compiler_params=pltpu.CompilerParams(collective_id=call_id, has_side_effects=True, vmem_limit_bytes=67000000),
    )(a_two, emis, init_row, end_pack, end_col)


def second_of(ranked, rows):
    batch = ranked.shape[0]
    alone = 2 * rows - batch
    return jnp.concatenate([jnp.zeros((alone,) + ranked.shape[1:], ranked.dtype), ranked[rows:][::-1]])


def solution(mesh):
    vec_axes = ('rows', 'states')

    def local_forward(trans_blk, emit_blk, init_blk, tokens, lengths):
        batch, n_steps = tokens.shape
        width = init_blk.shape[0]
        a_two = jnp.transpose(trans_blk, (1, 0, 2))
        table = emit_blk.T
        seq = jnp.arange(batch)
        longer = (lengths[None, :] > lengths[:, None]) | ((lengths[None, :] == lengths[:, None]) & (seq[None, :] < seq[:, None]))
        rank = jnp.sum(longer.astype(jnp.int32), axis=1)
        at_rank = rank[None, :] == seq[:, None]
        len_ranked = jnp.sum(jnp.where(at_rank, lengths[None, :], 0), axis=1)
        tok_ranked = jnp.sum(jnp.where(at_rank[:, :, None], tokens[None, :, :], 0), axis=1)

        def run(rows, call_id):
            def branch(a_two, table, init_blk, rank, len_ranked, tok_ranked):
                end_1 = len_ranked[:rows]
                end_2 = end_1 + second_of(len_ranked, rows)
                step = jnp.arange(n_steps)
                since = step[:, None] - end_1[None, :]
                later = jnp.sum(jnp.where(since[:, :, None] == step[None, None, :], second_of(tok_ranked, rows)[None, :, :], 0), axis=2)
                tok = jnp.where(since < 0, tok_ranked[:rows].T, later)
                emis = table.at[tok.reshape(-1)].get(mode='promise_in_bounds').reshape(n_steps, rows, width)
                ends = jnp.stack([end_1, end_2])
                packed = jnp.swapaxes(ends.reshape(2, rows // GROUP, GROUP), 1, 2)
                end_pack = jnp.pad(packed, ((0, 0), (0, 0), (0, LANES - rows // GROUP)))
                end_col = jnp.broadcast_to(ends[:, :, None], (2, rows, LANES))
                ll, alpha = run_forward(a_two, emis, init_blk[None, :], end_pack, end_col, 2 if rows < batch else 1, call_id)
                at = jnp.where(rank < rows, rank, 3 * rows - 1 - rank)
                ll_rows = jnp.swapaxes(ll[:, :, :rows // GROUP], 1, 2).reshape(2 * rows)
                loglik = jnp.sum(jnp.where(at[:, None] == jnp.arange(2 * rows)[None, :], ll_rows[None, :], 0.0), axis=1)
                return loglik, alpha.reshape(-1, width).at[at].get(mode='promise_in_bounds')

            return branch

        def fits(rows):
            return jnp.max(jnp.where(jnp.arange(rows) >= 2 * rows - batch, len_ranked[:rows] + second_of(len_ranked, rows), 0)) <= n_steps

        sizes = (40, 48, batch)
        pick = jnp.where(fits(40), 0, jnp.where(fits(48), 1, 2))
        return lax.switch(pick, [run(m, k) for k, m in enumerate(sizes)], a_two, table, init_blk, rank, len_ranked, tok_ranked)

    return jax.shard_map(local_forward, mesh=mesh, in_specs=(P('rows', None, 'states'), P(vec_axes, None), P(vec_axes), P('seqs', None), P('seqs')), out_specs=(P('seqs'), P('seqs', vec_axes)), check_vma=False)
```

```python
import functools

import jax
import jax.numpy as jnp
from jax import lax
from jax.experimental import pallas as pl
from jax.experimental.pallas import tpu as pltpu
from jax.sharding import PartitionSpec as P

MESH = pl.DeviceIdType.MESH
LANES = 128
GROUP = 8


def forward_kernel(
    n_steps, rows, width, piece, chunk, depth,
    a_hbm, emis_hbm, init_ref, end_pack, end_col,
    ll_ref, alpha_ref,
    held, ring, a_bf, gath, y_out, y_in, emis, c_buf, c_acc, inv_b,
    held_sem, ring_sem, emis_sem, y_ss, y_rs, x_ss, x_rs, p_ss, p_rs, f_ss, f_rs, c_ss, c_rs,
    credit_x, credit_p,
):
    n_pieces = width // piece
    n_chunks = width // chunk
    n_held_own = held.shape[0] - n_chunks
    per_chunk = chunk // piece
    k_parts = a_bf.shape[1] // depth
    row = lax.axis_index('rows')
    st = lax.axis_index('states')
    across = lax.rem(st + 2, 4)
    partner = st + 1 - 2 * lax.rem(st, 2)
    other = 1 - row
    me = row * 4 + st
    to_y = {'rows': other}
    to_x = {'states': across}
    to_p = {'states': partner}
    peers = []
    for k in range(1, 8):
        peers.append({'rows': lax.rem(row + k // 4, 2), 'states': lax.rem(st + k % 4, 4)})

    barrier = pltpu.get_barrier_semaphore()
    for peer in peers:
        pl.semaphore_signal(barrier, inc=1, device_id=peer, device_id_type=MESH)

    def held_copy(ch):
        half, c = (other, ch) if ch < n_chunks else (row, 2 * (ch - n_chunks) + 1)
        return pltpu.make_async_copy(a_hbm.at[half, :, pl.ds(c * chunk, chunk)], held.at[ch], held_sem.at[ch])

    def ring_copy(c, k):
        cols = pl.ds(pl.multiple_of(c * chunk, chunk), chunk)
        return pltpu.make_async_copy(a_hbm.at[row, pl.ds(k * depth, depth), cols], ring.at[k], ring_sem.at[k])

    def emis_copy(t, slot):
        return pltpu.make_async_copy(emis_hbm.at[t, pl.ds(0, rows)], emis.at[slot], emis_sem.at[slot])

    def remote(src, dst, ss, rs, dev):
        return pltpu.make_async_remote_copy(src_ref=src, dst_ref=dst, send_sem=ss, recv_sem=rs, device_id=dev, device_id_type=MESH)

    def y_copy(p):
        return remote(y_out.at[p], y_in.at[p], y_ss.at[p], y_rs.at[p], to_y)

    def own_slot(par):
        return st + par * (4 - st)

    def x_copy(p, par):
        return remote(gath.at[own_slot(par), p], gath.at[st, p], x_ss.at[p], x_rs.at[p], to_x)

    def x_arrived(p):
        return remote(gath.at[across, p], gath.at[across, p], x_ss.at[p], x_rs.at[p], to_x)

    def p_copy(p, par):
        return remote(gath.at[own_slot(par), p], gath.at[st, p], p_ss.at[p], p_rs.at[p], to_p)

    def p_arrived(p):
        return remote(gath.at[partner, p], gath.at[partner, p], p_ss.at[p], p_rs.at[p], to_p)

    def f_copy(p):
        return remote(gath.at[across, p], gath.at[across, p], f_ss.at[p], f_rs.at[p], to_p)

    def f_arrived(p):
        far = lax.rem(partner + 2, 4)
        return remote(gath.at[far, p], gath.at[far, p], f_ss.at[p], f_rs.at[p], to_p)

    def c_copy(par, k):
        return remote(c_buf.at[par, me], c_buf.at[par, me], c_ss.at[k], c_rs.at[par, k], peers[k - 1])

    def c_arrived(par, k):
        src = lax.rem(row + k // 4, 2) * 4 + lax.rem(st + 4 - k % 4, 4)
        return remote(c_buf.at[par, src], c_buf.at[par, src], c_ss.at[k], c_rs.at[par, k], peers[k - 1])

    emis_copy(0, 0).start()
    for ch in range(n_chunks - 2):
        held_copy(ch).start()
    emis_copy(1, 1).start()
    pl.semaphore_wait(barrier, 7)

    lane = lax.broadcasted_iota(jnp.int32, (GROUP, LANES), 1)
    ll_ref[...] = jnp.zeros_like(ll_ref)
    alpha_ref[...] = jnp.zeros_like(alpha_ref)

    def emit_piece(p, value, t, par):
        for j in range(piece // LANES):
            cols = pl.ds(pl.multiple_of(p * piece + j * LANES, LANES), LANES)
            fresh = jnp.broadcast_to(init_ref[:, cols], (rows, LANES))
            if value is not None:
                fresh = jnp.where(t == end_col[0], fresh, value[:, j * LANES:(j + 1) * LANES])
            r = fresh * emis[par, :, cols].astype(jnp.float32)
            gath[own_slot(par), p, :, j * LANES:(j + 1) * LANES] = r
            c_acc[...] += r
        x_copy(p, par).start()
        p_copy(p, par).start()

    def forward(p):
        x_arrived(p).wait_recv()
        f_copy(p).start()

    def capture(t):
        first = t < end_col[0]
        second = jnp.logical_and(jnp.logical_not(first), t < end_col[1])
        scale = inv_b[...]
        for p in range(n_pieces):
            for j in range(piece // LANES):
                cols = pl.ds(p * piece + j * LANES, LANES)
                a = gath[own_slot(lax.rem(t, 2)), p, :, j * LANES:(j + 1) * LANES] * scale
                alpha_ref[0, :, cols] = jnp.where(first, a, alpha_ref[0, :, cols])
                if alpha_ref.shape[0] > 1:
                    alpha_ref[1, :, cols] = jnp.where(second, a, alpha_ref[1, :, cols])

    def finish(t):
        par = lax.rem(t, 2)
        pack = jnp.zeros((GROUP, LANES), jnp.float32)
        for i in range(rows // GROUP):
            total = jnp.sum(c_acc[pl.ds(i * GROUP, GROUP), :], axis=1, keepdims=True)
            pack = jnp.where(lane == i, total, pack)
        c_buf[par, me] = pack
        for k in range(1, 8):
            c_copy(par, k).start()
        c_acc[...] = jnp.zeros_like(c_acc)
        if not isinstance(t, int):
            capture(t - 1)
        for p in range(n_pieces):
            forward(p)
        for k in range(1, 8):
            c_arrived(par, k).wait_recv()
        total = c_buf[par, 0]
        for k in range(1, 8):
            total = total + c_buf[par, k]
        log_c = jnp.log(total)
        first = t < end_pack[0]
        ll_ref[0] += jnp.where(first, log_c, 0.0)
        ll_ref[1] += jnp.where(jnp.logical_and(jnp.logical_not(first), t < end_pack[1]), log_c, 0.0)
        inv = 1.0 / total
        for i in range(rows // GROUP):
            inv_b[pl.ds(i * GROUP, GROUP), :] = jnp.broadcast_to(inv[:, i:i + 1], (GROUP, LANES))

        def convert(slot, src, p):
            scale = inv_b[...]
            for j in range(piece // LANES):
                at = pl.multiple_of(src * width + p * piece + j * LANES, LANES)
                a_bf[0:rows, pl.ds(at, LANES)] = (gath[slot, p, :, j * LANES:(j + 1) * LANES] * scale).astype(jnp.bfloat16)

        def convert_own(p, _):
            convert(own_slot(par), st, p)
            convert(across, across, p)
            return 0

        lax.fori_loop(0, n_pieces, convert_own, 0)

        def convert_near(p, _):
            p_arrived(p).wait_recv()
            f_arrived(p).wait_recv()
            convert(partner, partner, p)
            far = lax.rem(partner + 2, 4)
            convert(far, far, p)
            return 0

        lax.fori_loop(0, n_pieces, convert_near, 0)
        for p in range(n_pieces):
            x_copy(p, par).wait_send()
            p_copy(p, par).wait_send()
            f_copy(p).wait_send()
        for k in range(1, 8):
            c_copy(par, k).wait_send()

        @pl.when(t < n_steps - 1)
        def _():
            pl.semaphore_signal(credit_x, inc=1, device_id=to_x, device_id_type=MESH)
            pl.semaphore_signal(credit_p, inc=1, device_id=to_p, device_id_type=MESH)

    if a_bf.shape[0] > rows:
        a_bf[rows:, :] = jnp.zeros((a_bf.shape[0] - rows, a_bf.shape[1]), jnp.bfloat16)
    c_acc[...] = jnp.zeros_like(c_acc)
    emis_copy(0, 0).wait()
    for p in range(n_pieces):
        emit_piece(p, None, 0, 0)
    held_copy(n_chunks - 2).start()
    for k in range(k_parts):
        ring_copy(0, k).start()
    finish(0)
    for ch in range(n_chunks - 1, held.shape[0]):
        held_copy(ch).start()

    def one_step(t, _):
        par = lax.rem(t, 2)

        @pl.when(t + 1 < n_steps)
        def _():
            emis_copy(t + 1, 1 - par).start()

        def send_half(c, _):
            @pl.when(t == 1)
            def _():
                for ch in range(n_chunks):
                    @pl.when(c == ch)
                    def _():
                        held_copy(ch).wait()

            out = jnp.dot(a_bf[...], held[c], preferred_element_type=jnp.float32)[0:rows]
            for h in range(per_chunk):
                p = c * per_chunk + h
                y_out[p] = out[:, h * piece:(h + 1) * piece]
                y_copy(p).start()
            return 0

        lax.fori_loop(0, n_held_own, send_half, 0)
        pl.semaphore_wait(credit_x, 1)
        pl.semaphore_wait(credit_p, 1)
        emis_copy(t, par).wait()

        def pieces(c, out):
            for h in range(per_chunk):
                p = c * per_chunk + h
                y_copy(p).wait_recv()
                emit_piece(p, out[:, h * piece:(h + 1) * piece] + y_in[p], t, par)

        def own_pair(i, _):
            c = 2 * i
            lax.fori_loop(2 + 2 * i, 3 + i, send_half, 0)
            out = None
            for k in range(k_parts):
                ring_copy(c, k).wait()
                term = jnp.dot(a_bf[:, k * depth:(k + 1) * depth], ring[k], preferred_element_type=jnp.float32)[0:rows]
                out = term if out is None else out + term
                last = i == n_held_own - 1

                @pl.when(jnp.logical_not(last))
                def _():
                    ring_copy(c + 2, k).start()

                @pl.when(jnp.logical_and(last, t < n_steps - 1))
                def _():
                    ring_copy(0, k).start()

            pieces(c, out)
            lax.fori_loop(3 + i, n_chunks, send_half, 0)

            @pl.when(t == 1)
            def _():
                for ch in range(n_held_own):
                    @pl.when(i == ch)
                    def _():
                        held_copy(n_chunks + ch).wait()

            pieces(c + 1, jnp.dot(a_bf[...], held[n_chunks + i], preferred_element_type=jnp.float32)[0:rows])
            return 0

        lax.fori_loop(0, n_held_own, own_pair, 0)
        for p in range(n_pieces):
            y_copy(p).wait_send()
        finish(t)
        return 0

    lax.fori_loop(1, n_steps, one_step, 0)
    capture(n_steps - 1)


def run_forward(a_two, emis, init_row, end_pack, end_col, n_seqs, call_id):
    n_steps, rows, width = emis.shape
    piece, chunk, depth, n_held = 256, 512, 2048, 6
    sources = a_two.shape[1]
    n_pieces = width // piece
    dma = pltpu.SemaphoreType.DMA
    any_spec = pl.BlockSpec(memory_space=pl.ANY)
    vmem = pl.BlockSpec(memory_space=pltpu.VMEM)
    return pl.pallas_call(
        functools.partial(forward_kernel, n_steps, rows, width, piece, chunk, depth),
        out_shape=(jax.ShapeDtypeStruct((2, GROUP, LANES), jnp.float32), jax.ShapeDtypeStruct((n_seqs, rows, width), jnp.float32)),
        in_specs=[any_spec, any_spec, vmem, vmem, vmem],
        out_specs=(vmem, vmem),
        scratch_shapes=[
            pltpu.VMEM((n_held, sources, chunk), jnp.bfloat16),
            pltpu.VMEM((sources // depth, depth, chunk), jnp.bfloat16),
            pltpu.VMEM((128 if rows <= 48 else rows, sources), jnp.bfloat16),
            pltpu.VMEM((5, n_pieces, rows, piece), jnp.float32),
            pltpu.VMEM((n_pieces, rows, piece), jnp.float32),
            pltpu.VMEM((n_pieces, rows, piece), jnp.float32),
            pltpu.VMEM((2, rows, width), jnp.bfloat16),
            pltpu.VMEM((2, 8, GROUP, LANES), jnp.float32),
            pltpu.VMEM((rows, LANES), jnp.float32),
            pltpu.VMEM((rows, LANES), jnp.float32),
            dma((n_held,)), dma((sources // depth,)), dma((2,)),
            dma((n_pieces,)), dma((n_pieces,)), dma((n_pieces,)), dma((n_pieces,)),
            dma((n_pieces,)), dma((n_pieces,)), dma((n_pieces,)), dma((n_pieces,)),
            dma((8,)), dma((2, 8)),
            pltpu.SemaphoreType.REGULAR, pltpu.SemaphoreType.REGULAR,
        ],
        compiler_params=pltpu.CompilerParams(collective_id=call_id, has_side_effects=True, vmem_limit_bytes=67000000),
    )(a_two, emis, init_row, end_pack, end_col)


def second_of(ranked, rows):
    batch = ranked.shape[0]
    alone = 2 * rows - batch
    return jnp.concatenate([jnp.zeros((alone,) + ranked.shape[1:], ranked.dtype), ranked[rows:][::-1]])


def solution(mesh):
    vec_axes = ('rows', 'states')

    def local_forward(trans_blk, emit_blk, init_blk, tokens, lengths):
        batch, n_steps = tokens.shape
        width = init_blk.shape[0]
        a_two = jnp.transpose(trans_blk, (1, 0, 2))
        table = emit_blk.T
        seq = jnp.arange(batch)
        longer = (lengths[None, :] > lengths[:, None]) | ((lengths[None, :] == lengths[:, None]) & (seq[None, :] < seq[:, None]))
        rank = jnp.sum(longer.astype(jnp.int32), axis=1)
        at_rank = rank[None, :] == seq[:, None]
        len_ranked = jnp.sum(jnp.where(at_rank, lengths[None, :], 0), axis=1)
        tok_ranked = jnp.sum(jnp.where(at_rank[:, :, None], tokens[None, :, :], 0), axis=1)

        def run(rows, call_id):
            def branch(a_two, table, init_blk, rank, len_ranked, tok_ranked):
                end_1 = len_ranked[:rows]
                end_2 = end_1 + second_of(len_ranked, rows)
                step = jnp.arange(n_steps)
                since = step[:, None] - end_1[None, :]
                later = jnp.sum(jnp.where(since[:, :, None] == step[None, None, :], second_of(tok_ranked, rows)[None, :, :], 0), axis=2)
                tok = jnp.where(since < 0, tok_ranked[:rows].T, later)
                emis = table.at[tok.reshape(-1)].get(mode='promise_in_bounds').reshape(n_steps, rows, width)
                ends = jnp.stack([end_1, end_2])
                packed = jnp.swapaxes(ends.reshape(2, rows // GROUP, GROUP), 1, 2)
                end_pack = jnp.pad(packed, ((0, 0), (0, 0), (0, LANES - rows // GROUP)))
                end_col = jnp.broadcast_to(ends[:, :, None], (2, rows, LANES))
                ll, alpha = run_forward(a_two, emis, init_blk[None, :], end_pack, end_col, 2 if rows < batch else 1, call_id)
                at = jnp.where(rank < rows, rank, 3 * rows - 1 - rank)
                ll_rows = jnp.swapaxes(ll[:, :, :rows // GROUP], 1, 2).reshape(2 * rows)
                loglik = jnp.sum(jnp.where(at[:, None] == jnp.arange(2 * rows)[None, :], ll_rows[None, :], 0.0), axis=1)
                return loglik, alpha.reshape(-1, width).at[at].get(mode='promise_in_bounds')

            return branch

        def fits(rows):
            return jnp.max(jnp.where(jnp.arange(rows) >= 2 * rows - batch, len_ranked[:rows] + second_of(len_ranked, rows), 0)) <= n_steps

        sizes = (40, 48, batch)
        pick = jnp.where(fits(40), 0, jnp.where(fits(48), 1, 2))
        return lax.switch(pick, [run(m, k) for k, m in enumerate(sizes)], a_two, table, init_blk, rank, len_ranked, tok_ranked)

    return jax.shard_map(local_forward, mesh=mesh, in_specs=(P('rows', None, 'states'), P(vec_axes, None), P(vec_axes), P('seqs', None), P('seqs')), out_specs=(P('seqs'), P('seqs', vec_axes)), check_vma=False)
```
